32 devices in a mesh: tm: 4 (over y, core), space: 8 (over z, x).
Axes of the slice: x: 2, y: 2, z: 4, core: 2. Of those that a mesh axis runs over, the one named last changes fastest.
Arguments:
- perm_field: float32 [4, 32, 32, 256], P(None, 'space'), may hold values from 0.5 to 2
- step_multiplier: float32 [4, 32, 32, 256], P('tm', 'space'), may hold values from 0.5 to 2
- inflow: float32 [4, 32, 32, 256], P('tm', 'space'), may hold values from -3 to 3
- start_pressure: float32 [32, 32, 256], P('space'), may hold values from -6 to 6
- start_saturation: float32 [32, 32, 256], P('space'), may hold values from 0.1 to 0.9
- region_ids: int32 [32, 32, 256], P('space'), may hold values from 0 to 7
- region_table: float32 [3, 8], replicated, may hold values from 0.25 to 2
- well_cells: int32 [32], replicated, may hold values from 0 to 262143
- well_rates: float32 [4, 32], P('tm'), may hold values from -8 to 8
- observed: float32 [4, 4, 32], P(None, 'tm'), may hold values from -6 to 6
Outputs:
- misfit: float32 [4], replicated
- slab_pressure: float32 [4, 4, 32, 32, 256], P('tm', None, 'space')
- slab_saturation: float32 [4, 4, 32, 32, 256], P('tm', None, 'space')
The draws below stay inside these ranges and needn't reach their ends.
All inputs are finite; a program needn't handle non-finite values.
Results may differ from the reference program's by a relative error of at most 0.0003.
Values sent between devices are 32-bit elements; how exact they have to be, the bound alone decides.
A program may use at most 64 MiB of HBM per device.

```python
import math
import jax
import jax.numpy as jnp
from jax import lax

NZ = 32
NY = 256
REP_DEV = 1
ITERS = 3
WELLS = 32
REGIONS = 8
MEMBERS = 4
REPORTS = 4
NX = 32


def place_ends(entries, stream_key, low, largest):
    shape = entries.shape
    place = [jax.random.randint(jax.random.fold_in(stream_key, axis), (), 0, shape[axis]) for axis in range(len(shape))]
    entries = entries.at[tuple(place)].set(low)
    longest = shape.index(max(shape))
    place[longest] = (place[longest] + 1) % shape[longest]
    return entries.at[tuple(place)].set(largest)


def block_scale(key, extent, cuts, smallest, top_value):
    def one(dim, blocks):
        heights = jax.random.uniform(jax.random.fold_in(jax.random.fold_in(key, 6), dim), (blocks,), jnp.float32, smallest / len(cuts), top_value / len(cuts))
        return jnp.repeat(jnp.exp(heights), extent[dim] // blocks).reshape((-1,) + (1,) * (len(extent) - dim - 1))

    factor_of = one(*cuts[0])
    for cut in cuts[1:]:
        factor_of = factor_of * one(*cut)
    return factor_of


def bell_draw(rng, shape, scale, reach, shards=(), kind=jnp.bfloat16):
    values = scale * jax.random.normal(rng, shape, jnp.float32)
    if shards:
        values = values * block_scale(rng, shape, shards, -0.22, 0.18)
    return jnp.clip(values, -reach, reach).astype(kind)


def setup_inputs(seed: int = 0) -> dict:
    arg_keys = jax.random.split(jax.random.key(seed), 11)
    perm_field = jnp.clip(jnp.exp(math.log(2.0) - 1.3862944 * jax.random.uniform(arg_keys[0], (MEMBERS, NX, NZ, NY), jnp.float32) ** block_scale(arg_keys[0], (MEMBERS, NX, NZ, NY), ((1, 8),), -0.2, 0.2)), 0.5, 2.0)
    step_multiplier = jnp.clip(jnp.exp(math.log(2.0) - 1.3862944 * jax.random.uniform(arg_keys[1], (REPORTS, NX, NZ, NY), jnp.float32) ** block_scale(arg_keys[1], (REPORTS, NX, NZ, NY), ((0, 4), (1, 8)), -0.2, 0.2)), 0.5, 2.0)
    inflow = bell_draw(arg_keys[2], (REPORTS, NX, NZ, NY), 0.5, 3.0, ((0, 4), (1, 8)), jnp.float32)
    start_pressure = bell_draw(arg_keys[3], (NX, NZ, NY), 1.0, 6.0, ((0, 8),), jnp.float32)
    start_saturation = jnp.clip(0.1 + 0.79999997 * jax.random.uniform(arg_keys[4], (NX, NZ, NY), jnp.float32) ** block_scale(arg_keys[4], (NX, NZ, NY), ((0, 8),), -0.2, 0.2), 0.1, 0.9)
    region_ids = place_ends(jax.random.randint(arg_keys[5], (NX, NZ, NY), 0, REGIONS), jax.random.fold_in(arg_keys[5], 1), 0, REGIONS - 1).astype(jnp.int32)
    region_table = jnp.clip(jnp.exp(jax.random.uniform(arg_keys[6], (3, REGIONS), jnp.float32, math.log(0.25), math.log(2.0))), 0.25, 2.0)
    well_cells = place_ends(jax.random.randint(arg_keys[7], (WELLS,), 0, NX * NZ * NY), jax.random.fold_in(arg_keys[7], 1), 0, (NX * NZ * NY) - 1).astype(jnp.int32)
    well_rates = bell_draw(arg_keys[8], (REPORTS, WELLS), 2.0, 8.0, ((0, 4),), jnp.float32)
    observed = bell_draw(arg_keys[9], (MEMBERS, REPORTS, WELLS), 1.0, 6.0, ((1, 4),), jnp.float32)
    return {"perm_field": perm_field, "step_multiplier": step_multiplier, "inflow": inflow, "start_pressure": start_pressure, "start_saturation": start_saturation, "region_ids": region_ids, "region_table": region_table, "well_cells": well_cells, "well_rates": well_rates, "observed": observed}


def shifted(values, dimension, offset):
    margins = [(0, 0)] * values.ndim
    length = values.shape[dimension]
    if offset > 0:
        margins[dimension] = (1, 0)
        return lax.slice_in_dim(jnp.pad(values, margins), 0, length, axis=dimension)
    margins[dimension] = (0, 1)
    return lax.slice_in_dim(jnp.pad(values, margins), 1, length + 1, axis=dimension)

def neighbour_values(values_ext):
    middle = values_ext[:, 1:-1]
    return (values_ext[:, :-2], values_ext[:, 2:], shifted(middle, 2, 1), shifted(middle, 2, -1), shifted(middle, 3, 1), shifted(middle, 3, -1))

def coefficients(conduct_ext):
    middle = conduct_ext[:, 1:-1]
    others = neighbour_values(conduct_ext)
    links = [jnp.sqrt(middle * other_side) for other_side in others]
    link_total = links[0] + links[1] + links[2] + links[3] + links[4] + links[5]
    return tuple(links) + (link_total,)

def jacobi_sweep(pressure_ext, couplings, storage, right_side):
    beside = neighbour_values(pressure_ext)
    inflowing = couplings[0] * beside[0]
    for link_index in range(1, 6):
        inflowing = inflowing + couplings[link_index] * beside[link_index]
    divisor = jnp.where(storage > 0, storage + couplings[6], 1.0)
    return (right_side + inflowing) / divisor

def fraction(saturation, ratio):
    squared = saturation * saturation
    remain = (1.0 - saturation) * (1.0 - saturation)
    return squared / (squared + ratio * remain)

def transport(pressure_ext, flow_ext, couplings, saturation, gain, source):
    centre_p = pressure_ext[:, 1:-1]
    centre_f = flow_ext[:, 1:-1]
    other_p = neighbour_values(pressure_ext)
    other_f = neighbour_values(flow_ext)
    outflow = None
    for link_index in range(6):
        face_flux = couplings[link_index] * (centre_p - other_p[link_index])
        carried = face_flux * jnp.where(face_flux > 0, centre_f, other_f[link_index])
        outflow = carried if outflow is None else outflow + carried
    gained = jnp.maximum(source, 0.0) * (1.0 - saturation) - jnp.maximum(-source, 0.0) * centre_f - outflow
    return saturation + gain * gained

def region_fields(region_ids, region_table):
    fields = []
    for table_row in range(3):
        summed = jnp.zeros(region_ids.shape, jnp.float32)
        for region_index in range(region_table.shape[1]):
            summed = summed + jnp.where(region_ids == region_index, region_table[table_row, region_index], 0.0)
        fields.append(summed)
    return (fields[0], fields[1], 0.1 * fields[2])

def reference(perm_field, step_multiplier, inflow, start_pressure, start_saturation, region_ids, region_table, well_cells, well_rates, observed):
    storage, ratio, gain = region_fields(region_ids, region_table)
    pressure = jnp.broadcast_to(start_pressure, (MEMBERS,) + start_pressure.shape)
    saturation = jnp.broadcast_to(start_saturation, (MEMBERS,) + start_saturation.shape)
    misfit = jnp.zeros((MEMBERS,), jnp.float32)
    end_pressure = []
    end_saturation = []
    edges = ((0, 0), (1, 1), (0, 0), (0, 0))
    for report_index in range(REPORTS):
        source = jnp.zeros((NX * NZ * NY,), jnp.float32).at[well_cells].add(well_rates[report_index]).reshape(NX, NZ, NY)
        couplings = coefficients(jnp.pad(perm_field * step_multiplier[report_index], edges))
        right_side = storage * pressure + source + inflow[report_index]
        iterate = pressure
        for sweep_index in range(ITERS):
            iterate = jacobi_sweep(jnp.pad(iterate, edges), couplings, storage, right_side)
        flow_frac = fraction(saturation, ratio)
        saturation = transport(jnp.pad(iterate, edges), jnp.pad(flow_frac, edges), couplings, saturation, gain, source)
        pressure = iterate
        predicted = pressure.reshape(MEMBERS, -1)[:, well_cells]
        misfit = misfit + lax.optimization_barrier(jnp.sum((predicted - observed[:, report_index]) ** 2, axis=1))
        if (report_index + 1) % REP_DEV == 0:
            end_pressure.append(pressure)
            end_saturation.append(saturation)
    return (misfit / (REPORTS * WELLS), jnp.stack(end_pressure), jnp.stack(end_saturation))
```

```python
import functools

import jax
import jax.numpy as jnp
from jax import lax
from jax.experimental import pallas as pl
from jax.experimental.pallas import tpu as pltpu
from jax.sharding import PartitionSpec as P

ITERS = 3
MESH = pl.DeviceIdType.MESH
EXACT = lax.Precision.HIGHEST


def before(v, axis):
    return pltpu.roll(v, 1, axis)


def after(v, axis):
    return pltpu.roll(v, v.shape[axis] - 1, axis)


def kernel(
    T, N,
    perm, mult, infl, p0, s0, ids, table, small, rows_row,
    mis, outp, outs,
    M, I, SM, MH, PH, HP, HF, PB, SB, FE, TX, TZP, TZM, TYP, TYM, RC, C, V, G, B, Q, E0, E1, E2, ES,
    sM, rM, sI, rI, sS, rS, sMH, rMH, sPH, rPH, sHP, rHP, sHF, rHF, sO, rO, lO, s1, r1, s2, r2,
):
    t = lax.axis_index("tm")
    i = lax.axis_index("space")
    X, Z, Y = p0.shape
    R = T
    W = small.shape[0]
    K = R * ITERS
    has = (i > 0, i < N - 1)
    beside = (i - 1, i + 1)
    edge = (0, X - 1)
    order = [0, X - 1] + list(range(1, X - 1))

    def rdma(src, dst, ss, rs, dev):
        return pltpu.make_async_remote_copy(
            src_ref=src, dst_ref=dst, send_sem=ss, recv_sem=rs, device_id=dev, device_id_type=MESH
        )

    def halo(side, src, dst_slots, ss, rs, peer=None):
        return rdma(
            src, dst_slots.at[1 - side], ss.at[side], rs.at[1 - side],
            (t if peer is None else peer, beside[side]),
        )

    def send_edge(side, src, slots, ss, rs, peer=None):
        @pl.when(has[side])
        def _():
            halo(side, src, slots, ss, rs, peer).start()

    def edge_sent(side, src, slots, ss, rs, peer=None):
        @pl.when(has[side])
        def _():
            halo(side, src, slots, ss, rs, peer).wait_send()

    def edge_here(side, slots, ss, rs):
        @pl.when(has[side])
        def _():
            rdma(slots.at[side], slots.at[side], ss.at[side], rs.at[side], (t, beside[side])).wait_recv()

    def peers():
        return [(d, lax.rem(t + d, T)) for d in range(1, T)]

    for side in (0, 1):
        send_edge(side, p0.at[edge[side]], HP.at[0], sHP.at[0], rHP.at[0])
        send_edge(side, perm.at[t, edge[side]], PH, sPH, rPH)
        send_edge(side, mult.at[0, edge[side]], MH.at[t], sMH.at[0], rMH.at[t])
    for d, peer in peers():
        rdma(small, SM.at[t], sS.at[d], rS.at[t], (peer, i)).start()
        rdma(mult.at[0], M.at[t], sM.at[d], rM.at[t], (peer, i)).start()
        for side in (0, 1):
            send_edge(side, mult.at[0, edge[side]], MH.at[t], sMH.at[d], rMH.at[t], peer)
    for d, peer in peers():
        rdma(infl.at[0], I.at[t], sI.at[d], rI.at[t], (peer, i)).start()

    for side in (0, 1):
        @pl.when(jnp.logical_not(has[side]))
        def _():
            zero = jnp.zeros((Z, Y), jnp.float32)
            PH[side] = zero

            def clear(n, c):
                HP[n, side] = zero
                return c

            lax.fori_loop(0, K + 1, clear, 0)

            def clear_r(n, c):
                HF[n, side] = zero
                MH[n, side] = zero
                return c

            lax.fori_loop(0, R, clear_r, 0)

    M[t] = mult[0]
    I[t] = infl[0]
    SM[t] = small[...]
    PB[0] = p0[...]
    SB[0] = s0[...]

    def fraction(s, v):
        sq = s * s
        rest = (1.0 - s) * (1.0 - s)
        return sq / (sq + v * rest)

    for x in order:
        rock = ids[x]
        c = jnp.zeros((Z, Y), jnp.float32)
        v = c
        g = c
        for k in range(table.shape[1]):
            hit = rock == k
            c = jnp.where(hit, table[0, k], c)
            v = jnp.where(hit, table[1, k], v)
            g = jnp.where(hit, table[2, k], g)
        C[x] = c
        V[x] = v
        G[x] = 0.1 * g
        FE[0, x] = fraction(s0[x], v)
    for side in (0, 1):
        send_edge(side, FE.at[0, edge[side]], HF.at[0], sHF.at[0], rHF.at[0])

    lane = lax.broadcasted_iota(jnp.int32, (W, small.shape[1]), 1)

    def column(block, n):
        return jnp.sum(jnp.where(lane == n, block, 0.0), axis=1, keepdims=True)

    base = (i * (X * Z)).astype(jnp.float32)
    local_col = column(small[...], T + 1) - base
    cols = column(small[...], T + 2)
    pick_rows = jnp.where(
        lax.broadcasted_iota(jnp.int32, (W, X * Z), 1).astype(jnp.float32) == local_col, 1.0, 0.0
    )
    pick_cols = jnp.where(
        lax.broadcasted_iota(jnp.int32, (W, Y), 1).astype(jnp.float32) == cols, 1.0, 0.0
    )
    put_rows = jnp.where(
        lax.broadcasted_iota(jnp.int32, (X * Z, W), 0).astype(jnp.float32) == rows_row[...] - base,
        1.0, 0.0,
    )
    owned = jnp.sum(pick_rows, axis=1, keepdims=True)

    def tm_here(r, buf, ss, rs):
        @pl.when(r != t)
        def _():
            rdma(buf.at[r], buf.at[r], ss.at[1], rs.at[r], (r, i)).wait_recv()

    zi = lax.broadcasted_iota(jnp.int32, (Z, Y), 0)
    yi = lax.broadcasted_iota(jnp.int32, (Z, Y), 1)

    def coef(r):
        slot = lax.rem(r, 2)
        tm_here(r, SM, sS, rS)
        tm_here(r, M, sM, rM)
        for side in (0, 1):
            edge_here(side, MH.at[r], sMH.at[0], rMH.at[r])
        a = [PH[0] * MH[r, 0]] + [perm[t, x] * M[r, x] for x in range(X)] + [PH[1] * MH[r, 1]]
        for x in range(X + 1):
            TX[slot, x] = jnp.sqrt(a[x] * a[x + 1])
        for x in range(X):
            mid = a[x + 1]
            zp = jnp.where(zi < Z - 1, jnp.sqrt(mid * after(mid, 0)), 0.0)
            yp = jnp.where(yi < Y - 1, jnp.sqrt(mid * after(mid, 1)), 0.0)
            zm = before(zp, 0)
            ym = before(yp, 1)
            TZP[slot, x] = zp
            TZM[slot, x] = zm
            TYP[slot, x] = yp
            TYM[slot, x] = ym
            RC[slot, x] = 1.0 / (C[x] + (TX[slot, x] + TX[slot, x + 1] + zp + zm + yp + ym))
        rate = column(SM[r], 0)
        Q[slot] = jnp.dot(put_rows, pick_cols * rate, precision=EXACT).reshape(X, Z, Y)

    def start_step(r):
        slot = lax.rem(r, 2)
        tm_here(r, I, sI, rI)
        for x in range(X):
            B[x] = C[x] * PB[r * ITERS, x] + Q[slot, x] + I[r, x]

    def sweep(r, k):
        slot = lax.rem(r, 2)
        for n, x in enumerate(order):
            if x == 0:
                edge_here(0, HP.at[k], sHP.at[k], rHP.at[k])
                left = HP[k, 0]
            else:
                left = PB[k, x - 1]
            if x == X - 1:
                edge_here(1, HP.at[k], sHP.at[k], rHP.at[k])
                right = HP[k, 1]
            else:
                right = PB[k, x + 1]
            p = PB[k, x]
            total = B[x] + TX[slot, x] * left + TX[slot, x + 1] * right
            total = total + TZP[slot, x] * after(p, 0) + TZM[slot, x] * before(p, 0)
            total = total + TYP[slot, x] * after(p, 1) + TYM[slot, x] * before(p, 1)
            PB[k + 1, x] = total * RC[slot, x]
            if n < 2:
                send_edge(n, PB.at[k + 1, x], HP.at[k + 1], sHP.at[k + 1], rHP.at[k + 1])

    def put_out(r, src, out, which):
        @pl.when(r != t)
        def _():
            rdma(src, out.at[0, t], sO.at[r, which], rO.at[t, which], (r, i)).start()

        @pl.when(r == t)
        def _():
            pltpu.make_async_copy(src, out.at[0, t], lO.at[which]).start()

    def transport(r):
        slot = lax.rem(r, 2)
        k = (r + 1) * ITERS
        for side in (0, 1):
            edge_here(side, HF.at[r], sHF.at[r], rHF.at[r])

        def face(coupling, pi, pj, fi, fj):
            flux = coupling * (pi - pj)
            return flux * jnp.where(flux > 0, fi, fj)

        def p_of(x):
            return HP[k, 0] if x < 0 else (HP[k, 1] if x >= X else PB[k, x])

        def f_of(x):
            return HF[r, 0] if x < 0 else (HF[r, 1] if x >= X else FE[r, x])

        for x in order:
            p = p_of(x)
            f = f_of(x)
            s = SB[r, x]
            q = Q[slot, x]
            out = face(TX[slot, x + 1], p, p_of(x + 1), f, f_of(x + 1))
            out = out - face(TX[slot, x], p_of(x - 1), p, f_of(x - 1), f)
            cz = face(TZP[slot, x], p, after(p, 0), f, after(f, 0))
            cy = face(TYP[slot, x], p, after(p, 1), f, after(f, 1))
            out = out + (cz - before(cz, 0)) + (cy - before(cy, 1))
            gained = jnp.maximum(q, 0.0) * (1.0 - s) - jnp.maximum(-q, 0.0) * f - out
            s = s + G[x] * gained
            SB[r + 1, x] = s
            FE[r + 1, x] = fraction(s, V[x])
        put_out(r, SB.at[r + 1], outs, 1)

        @pl.when(r < R - 1)
        def _():
            for side in (0, 1):
                send_edge(side, FE.at[r + 1, edge[side]], HF.at[r + 1], sHF.at[r + 1], rHF.at[r + 1])

    for side in (0, 1):
        edge_here(side, PH, sPH, rPH)
    coef(0)
    ES[...] = jnp.zeros(ES.shape, jnp.float32)

    def step(r, carry):
        k = r * ITERS
        start_step(r)
        sweep(r, k)

        @pl.when(r > 0)
        def _():
            transport(r - 1)

        for j in range(1, ITERS):
            sweep(r, k + j)
            if j == 1:
                @pl.when(r < R - 1)
                def _():
                    coef(r + 1)
        put_out(r, PB.at[k + ITERS], outp, 0)
        seen = jnp.dot(pick_rows, PB[k + ITERS].reshape(X * Z, Y), precision=EXACT)
        predicted = jnp.sum(seen * pick_cols, axis=1, keepdims=True)
        gap = predicted - column(SM[r], 1 + t)
        ES[...] = ES[...] + owned * gap * gap
        return carry

    lax.fori_loop(0, R, step, 0)

    E0[...] = jnp.broadcast_to(jnp.sum(ES[...], axis=0, keepdims=True), E0.shape)
    others = [(d, lax.rem(i + d, N)) for d in range(1, N)]
    for d, peer in others:
        rdma(E0, E1.at[i], s1.at[d], r1.at[i], (t, peer)).start()
    for side in (0, 1):
        edge_here(side, HP.at[K], sHP.at[K], rHP.at[K])
    transport(R - 1)
    E1[i] = E0[...]
    for d, peer in others:
        rdma(E1.at[peer], E1.at[peer], s1.at[d], r1.at[peer], (t, peer)).wait_recv()
    whole = E1[0]
    for n in range(1, N):
        whole = whole + E1[n]
    mine = lax.broadcasted_iota(jnp.int32, whole.shape, 1) == t
    E2[t] = jnp.where(mine, whole, 0.0)
    for d, peer in peers():
        rdma(E2.at[t], E2.at[t], s2.at[d], r2.at[t], (peer, i)).start()
    for d, peer in peers():
        rdma(E2.at[peer], E2.at[peer], s2.at[d], r2.at[peer], (peer, i)).wait_recv()
    result = E2[0]
    for n in range(1, T):
        result = result + E2[n]
    mis[...] = result * (1.0 / (R * W))

    for side in (0, 1):
        edge_sent(side, p0.at[edge[side]], HP.at[0], sHP.at[0], rHP.at[0])
        edge_sent(side, perm.at[t, edge[side]], PH, sPH, rPH)
        edge_sent(side, mult.at[0, edge[side]], MH.at[t], sMH.at[0], rMH.at[t])

        def sent_k(k, c):
            edge_sent(side, PB.at[k, edge[side]], HP.at[k], sHP.at[k], rHP.at[k])
            return c

        lax.fori_loop(1, K + 1, sent_k, 0)

        def sent_r(r, c):
            edge_sent(side, FE.at[r, edge[side]], HF.at[r], sHF.at[r], rHF.at[r])
            return c

        lax.fori_loop(0, R, sent_r, 0)
    for d, peer in peers():
        rdma(small, SM.at[t], sS.at[d], rS.at[t], (peer, i)).wait_send()
        rdma(mult.at[0], M.at[t], sM.at[d], rM.at[t], (peer, i)).wait_send()
        rdma(infl.at[0], I.at[t], sI.at[d], rI.at[t], (peer, i)).wait_send()
        rdma(E2.at[t], E2.at[t], s2.at[d], r2.at[t], (peer, i)).wait_send()
        for side in (0, 1):
            edge_sent(side, mult.at[0, edge[side]], MH.at[t], sMH.at[d], rMH.at[t], peer)
    for d, peer in others:
        rdma(E0, E1.at[i], s1.at[d], r1.at[i], (t, peer)).wait_send()
    for d, peer in peers():
        for which, (src, out) in enumerate(((PB.at[K], outp), (SB.at[R], outs))):
            rdma(src, out.at[0, t], sO.at[peer, which], rO.at[t, which], (peer, i)).wait_send()
            rdma(src, out.at[0, peer], sO.at[peer, which], rO.at[peer, which], (peer, i)).wait_recv()
    for which, (src, out) in enumerate(((PB.at[K], outp), (SB.at[R], outs))):
        pltpu.make_async_copy(src, out.at[0, t], lO.at[which]).wait()


def body(
    perm_field, step_multiplier, inflow, start_pressure, start_saturation,
    region_ids, region_table, well_cells, well_rates, observed,
):
    T = lax.axis_size("tm")
    N = lax.axis_size("space")
    X, Z, Y = start_pressure.shape
    W = well_cells.shape[0]
    members = perm_field.shape[0]
    assert members == T and step_multiplier.shape[0] == 1
    well_row = (well_cells // Y).astype(jnp.float32)
    well_col = (well_cells % Y).astype(jnp.float32)
    small = jnp.concatenate(
        [well_rates, observed[:, 0, :], well_row[None], well_col[None]], axis=0
    ).T
    small = jnp.pad(small, ((0, 0), (0, 128 - small.shape[1])))
    K = T * ITERS
    f32 = jnp.float32
    cell = (Z, Y)
    block = (X, Z, Y)

    def buf(*shape):
        return pltpu.VMEM(shape, f32)

    dma = pltpu.SemaphoreType.DMA
    vmem = pl.BlockSpec(memory_space=pltpu.VMEM)
    anyspace = pl.BlockSpec(memory_space=pl.ANY)
    out_shape = jax.ShapeDtypeStruct((1, members) + block, f32)
    mis, outp, outs = pl.pallas_call(
        functools.partial(kernel, T, N),
        out_shape=(jax.ShapeDtypeStruct((8, 128), f32), out_shape, out_shape),
        in_specs=[vmem] * 6 + [pl.BlockSpec(memory_space=pltpu.SMEM)] + [vmem] * 2,
        out_specs=(vmem, anyspace, anyspace),
        scratch_shapes=[
            buf(T, *block), buf(T, *block), buf(T, W, 128), buf(T, 2, *cell), buf(2, *cell),
            buf(K + 1, 2, *cell), buf(T, 2, *cell), buf(K + 1, *block), buf(T + 1, *block),
            buf(T + 1, *block), buf(2, X + 1, *cell), buf(2, *block), buf(2, *block),
            buf(2, *block), buf(2, *block), buf(2, *block), buf(*block), buf(*block), buf(*block),
            buf(*block), buf(2, *block), buf(8, 128), buf(N, 8, 128), buf(T, 8, 128), buf(W, 1),
            dma((T,)), dma((T,)), dma((T,)), dma((T,)), dma((T,)), dma((T,)),
            dma((T, 2)), dma((T, 2)), dma((2,)), dma((2,)), dma((K + 1, 2)), dma((K + 1, 2)),
            dma((T, 2)), dma((T, 2)), dma((T, 2)), dma((T, 2)), dma((2,)),
            dma((N,)), dma((N,)), dma((T,)), dma((T,)),
        ],
        compiler_params=pltpu.CompilerParams(
            has_side_effects=True, vmem_limit_bytes=40 * 1024 * 1024
        ),
    )(
        perm_field, step_multiplier, inflow, start_pressure, start_saturation, region_ids,
        region_table, small, well_row[None],
    )
    return mis[0, :members], outp, outs


def solution(mesh):
    return jax.shard_map(
        body,
        mesh=mesh,
        in_specs=(
            P(None, "space", None, None),
            P("tm", "space", None, None),
            P("tm", "space", None, None),
            P("space", None, None),
            P("space", None, None),
            P("space", None, None),
            P(),
            P(),
            P("tm", None),
            P(None, "tm", None),
        ),
        out_specs=(P(), P("tm", None, "space", None, None), P("tm", None, "space", None, None)),
        check_vma=False,
    )
```

```python
import functools

import jax
import jax.numpy as jnp
from jax import lax
from jax.experimental import pallas as pl
from jax.experimental.pallas import tpu as pltpu
from jax.sharding import PartitionSpec as P

ITERS = 3
MESH = pl.DeviceIdType.MESH
EXACT = lax.Precision.HIGHEST


def before(v, axis):
    return pltpu.roll(v, 1, axis)


def after(v, axis):
    return pltpu.roll(v, v.shape[axis] - 1, axis)


def kernel(
    T, N,
    perm, mult, infl, p0, s0, ids, table, small, rows_row,
    mis, outp, outs,
    PM, IDS, M, I, SM, MH, PH, HP, HF, PB, SB, FE, TX, TZP, TZM, TYP, TYM, RC, C, V, G, B, Q, E0, E1, E2, ES,
    sM, rM, sI, rI, sS, rS, sMH, rMH, sPH, rPH, sHP, rHP, sHF, rHF, sO, rO, lO, s1, r1, s2, r2,
    fM, fI, fMH, lIN,
):
    t = lax.axis_index("tm")
    i = lax.axis_index("space")
    X, Z, Y = IDS.shape
    R = T
    loads = [
        pltpu.make_async_copy(src, dst, lIN.at[n])
        for n, (src, dst) in enumerate((
            (mult.at[0], M.at[t]), (p0, PB.at[0]), (perm.at[t], PM), (infl.at[0], I.at[t]),
            (ids, IDS), (s0, SB.at[0]),
        ))
    ]
    for load in loads:
        load.start()
    W = small.shape[0]
    K = R * ITERS
    has = (i > 0, i < N - 1)
    beside = (i - 1, i + 1)
    edge = (0, X - 1)
    order = [0, X - 1] + list(range(1, X - 1))

    def rdma(src, dst, ss, rs, dev):
        return pltpu.make_async_remote_copy(
            src_ref=src, dst_ref=dst, send_sem=ss, recv_sem=rs, device_id=dev, device_id_type=MESH
        )

    def halo(side, src, dst_slots, ss, rs, peer=None):
        return rdma(
            src, dst_slots.at[1 - side], ss.at[side], rs.at[1 - side],
            (t if peer is None else peer, beside[side]),
        )

    def send_edge(side, src, slots, ss, rs, peer=None):
        @pl.when(has[side])
        def _():
            halo(side, src, slots, ss, rs, peer).start()

    def edge_sent(side, src, slots, ss, rs, peer=None):
        @pl.when(has[side])
        def _():
            halo(side, src, slots, ss, rs, peer).wait_send()

    def edge_here(side, slots, ss, rs):
        @pl.when(has[side])
        def _():
            rdma(slots.at[side], slots.at[side], ss.at[side], rs.at[side], (t, beside[side])).wait_recv()

    def peers():
        return [(d, lax.rem(t + d, T)) for d in range(1, T)]

    barrier = pltpu.get_barrier_semaphore()

    def greet(device):
        pl.semaphore_signal(barrier, inc=1, device_id=device, device_id_type=MESH)

    for d, peer in peers():
        greet((peer, i))
    for d in range(1, N):
        greet((t, lax.rem(i + d, N)))
    for side in (0, 1):
        @pl.when(has[side])
        def _():
            for d, peer in peers():
                greet((peer, beside[side]))

    sides = jnp.where(has[0], 1, 0) + jnp.where(has[1], 1, 0)
    pl.semaphore_wait(barrier, (N - 1) + (T - 1) + (T - 1) * sides)

    mate = t + 1 - 2 * lax.rem(t, 2)

    def targets():
        return [(0, mate)] + [(d, lax.rem(t + 2 * d, T)) for d in range(1, T // 2)]

    def send_fields():
        for d, peer in targets():
            rdma(M.at[t], M.at[t], sM.at[d], rM.at[t], (peer, i)).start()
        for side in (0, 1):
            for d, peer in targets():
                send_edge(side, M.at[t, edge[side]], MH.at[t], sMH.at[d + 1], rMH.at[t], peer)
        for d, peer in targets():
            rdma(I.at[t], I.at[t], sI.at[d], rI.at[t], (peer, i)).start()

    def passes_on(r):
        return jnp.logical_and(lax.rem(t, 2) == lax.rem(r, 2), t != r)

    def pass_on(r):
        @pl.when(passes_on(r))
        def _():
            rdma(M.at[r], M.at[r], sM.at[1], rM.at[r], (r, i)).wait_recv()
            rdma(M.at[r], M.at[r], fM.at[r], rM.at[r], (mate, i)).start()
            for side in (0, 1):
                edge_here(side, MH.at[r], sMH.at[0], rMH.at[r])

                @pl.when(has[side])
                def _():
                    rdma(
                        MH.at[r, side], MH.at[r, side], fMH.at[r, side], rMH.at[r, side], (mate, i)
                    ).start()
            rdma(I.at[r], I.at[r], sI.at[1], rI.at[r], (r, i)).wait_recv()
            rdma(I.at[r], I.at[r], fI.at[r], rI.at[r], (mate, i)).start()

    for n in range(3):
        loads[n].wait()
    for side in (0, 1):
        send_edge(side, M.at[t, edge[side]], MH.at[t], sMH.at[0], rMH.at[t])
    loads[3].wait()

    @pl.when(t == 0)
    def _():
        send_fields()

    for side in (0, 1):
        send_edge(side, PM.at[edge[side]], PH, sPH, rPH)
        send_edge(side, PB.at[0, edge[side]], HP.at[0], sHP.at[0], rHP.at[0])
    for d, peer in peers():
        rdma(small, SM.at[t], sS.at[d], rS.at[t], (peer, i)).start()

    for side in (0, 1):
        @pl.when(jnp.logical_not(has[side]))
        def _():
            zero = jnp.zeros((Z, Y), jnp.float32)
            PH[side] = zero

            def clear(n, c):
                HP[n, side] = zero
                return c

            lax.fori_loop(0, K + 1, clear, 0)

            def clear_r(n, c):
                HF[n, side] = zero
                MH[n, side] = zero
                return c

            lax.fori_loop(0, R, clear_r, 0)

    SM[t] = small[...]
    loads[4].wait()
    loads[5].wait()

    def fraction(s, v):
        sq = s * s
        rest = (1.0 - s) * (1.0 - s)
        return sq / (sq + v * rest)

    for x in order:
        rock = IDS[x]
        c = jnp.zeros((Z, Y), jnp.float32)
        v = c
        g = c
        for k in range(table.shape[1]):
            hit = rock == k
            c = jnp.where(hit, table[0, k], c)
            v = jnp.where(hit, table[1, k], v)
            g = jnp.where(hit, table[2, k], g)
        C[x] = c
        V[x] = v
        G[x] = 0.1 * g
        FE[0, x] = fraction(SB[0, x], v)
    for side in (0, 1):
        send_edge(side, FE.at[0, edge[side]], HF.at[0], sHF.at[0], rHF.at[0])

    lane = lax.broadcasted_iota(jnp.int32, (W, small.shape[1]), 1)

    def column(block, n):
        return jnp.sum(jnp.where(lane == n, block, 0.0), axis=1, keepdims=True)

    base = (i * (X * Z)).astype(jnp.float32)
    local_col = column(small[...], T + 1) - base
    cols = column(small[...], T + 2)
    pick_rows = jnp.where(
        lax.broadcasted_iota(jnp.int32, (W, X * Z), 1).astype(jnp.float32) == local_col, 1.0, 0.0
    )
    pick_cols = jnp.where(
        lax.broadcasted_iota(jnp.int32, (W, Y), 1).astype(jnp.float32) == cols, 1.0, 0.0
    )
    put_rows = jnp.where(
        lax.broadcasted_iota(jnp.int32, (X * Z, W), 0).astype(jnp.float32) == rows_row[...] - base,
        1.0, 0.0,
    )
    owned = jnp.sum(pick_rows, axis=1, keepdims=True)

    def tm_here(r, buf, ss, rs):
        @pl.when(r != t)
        def _():
            rdma(buf.at[r], buf.at[r], ss.at[1], rs.at[r], (r, i)).wait_recv()

    zi = lax.broadcasted_iota(jnp.int32, (Z, Y), 0)
    yi = lax.broadcasted_iota(jnp.int32, (Z, Y), 1)

    def coef(r):
        slot = lax.rem(r, 2)
        tm_here(r, SM, sS, rS)

        @pl.when(jnp.logical_not(passes_on(r)))
        def _():
            tm_here(r, M, sM, rM)
            for side in (0, 1):
                edge_here(side, MH.at[r], sMH.at[0], rMH.at[r])

        a = [PH[0] * MH[r, 0]] + [PM[x] * M[r, x] for x in range(X)] + [PH[1] * MH[r, 1]]
        for x in range(X + 1):
            TX[slot, x] = jnp.sqrt(a[x] * a[x + 1])
        for x in range(X):
            mid = a[x + 1]
            zp = jnp.where(zi < Z - 1, jnp.sqrt(mid * after(mid, 0)), 0.0)
            yp = jnp.where(yi < Y - 1, jnp.sqrt(mid * after(mid, 1)), 0.0)
            zm = before(zp, 0)
            ym = before(yp, 1)
            TZP[slot, x] = zp
            TZM[slot, x] = zm
            TYP[slot, x] = yp
            TYM[slot, x] = ym
            RC[slot, x] = 1.0 / (C[x] + (TX[slot, x] + TX[slot, x + 1] + zp + zm + yp + ym))
        rate = column(SM[r], 0)
        Q[slot] = jnp.dot(put_rows, pick_cols * rate, precision=EXACT).reshape(X, Z, Y)

    def start_step(r):
        slot = lax.rem(r, 2)

        @pl.when(jnp.logical_not(passes_on(r)))
        def _():
            tm_here(r, I, sI, rI)

        for x in range(X):
            B[x] = C[x] * PB[r * ITERS, x] + Q[slot, x] + I[r, x]

    def sweep(r, k):
        slot = lax.rem(r, 2)
        for n, x in enumerate(order):
            if x == 0:
                edge_here(0, HP.at[k], sHP.at[k], rHP.at[k])
                left = HP[k, 0]
            else:
                left = PB[k, x - 1]
            if x == X - 1:
                edge_here(1, HP.at[k], sHP.at[k], rHP.at[k])
                right = HP[k, 1]
            else:
                right = PB[k, x + 1]
            p = PB[k, x]
            total = B[x] + TX[slot, x] * left + TX[slot, x + 1] * right
            total = total + TZP[slot, x] * after(p, 0) + TZM[slot, x] * before(p, 0)
            total = total + TYP[slot, x] * after(p, 1) + TYM[slot, x] * before(p, 1)
            PB[k + 1, x] = total * RC[slot, x]
            if n < 2:
                send_edge(n, PB.at[k + 1, x], HP.at[k + 1], sHP.at[k + 1], rHP.at[k + 1])

    parts = ((0, 0, X), (1, 1, X - 2), (2, 0, 1), (3, X - 1, 1))

    def piece(which, r, member):
        _, at, many = parts[which]
        rows = pl.ds(at, many)
        if which == 0:
            return PB.at[(r + 1) * ITERS, rows], outp.at[0, member, rows]
        return SB.at[r + 1, rows], outs.at[0, member, rows]

    def put_out(r, which):
        src, dst = piece(which, r, t)

        @pl.when(r != t)
        def _():
            rdma(src, dst, sO.at[r, which], rO.at[t, which], (r, i)).start()

        @pl.when(r == t)
        def _():
            pltpu.make_async_copy(src, dst, lO.at[which]).start()

    def transport(r, last=False):
        slot = lax.rem(r, 2)
        k = (r + 1) * ITERS
        def face(coupling, pi, pj, fi, fj):
            flux = coupling * (pi - pj)
            return flux * jnp.where(flux > 0, fi, fj)

        def p_of(x):
            return HP[k, 0] if x < 0 else (HP[k, 1] if x >= X else PB[k, x])

        def f_of(x):
            return HF[r, 0] if x < 0 else (HF[r, 1] if x >= X else FE[r, x])

        for x in order[2:] + order[:2]:
            if x in edge:
                side = edge.index(x)
                if side == 0:
                    put_out(r, 1)
                edge_here(side, HF.at[r], sHF.at[r], rHF.at[r])
                if last:
                    edge_here(side, HP.at[k], sHP.at[k], rHP.at[k])
            p = p_of(x)
            f = f_of(x)
            s = SB[r, x]
            q = Q[slot, x]
            out = face(TX[slot, x + 1], p, p_of(x + 1), f, f_of(x + 1))
            out = out - face(TX[slot, x], p_of(x - 1), p, f_of(x - 1), f)
            cz = face(TZP[slot, x], p, after(p, 0), f, after(f, 0))
            cy = face(TYP[slot, x], p, after(p, 1), f, after(f, 1))
            out = out + (cz - before(cz, 0)) + (cy - before(cy, 1))
            gained = jnp.maximum(q, 0.0) * (1.0 - s) - jnp.maximum(-q, 0.0) * f - out
            s = s + G[x] * gained
            SB[r + 1, x] = s
            if not last:
                FE[r + 1, x] = fraction(s, V[x])
            if x in edge:
                put_out(r, 2 + edge.index(x))

        @pl.when(r < R - 1)
        def _():
            for side in (0, 1):
                send_edge(side, FE.at[r + 1, edge[side]], HF.at[r + 1], sHF.at[r + 1], rHF.at[r + 1])

    pass_on(0)

    @pl.when(t > 0)
    def _():
        send_fields()

    for side in (0, 1):
        edge_here(side, PH, sPH, rPH)
    coef(0)
    ES[...] = jnp.zeros(ES.shape, jnp.float32)

    def step(r, carry):
        k = r * ITERS
        start_step(r)
        sweep(r, k)

        @pl.when(r > 0)
        def _():
            transport(r - 1)

        @pl.when(r < R - 1)
        def _():
            pass_on(r + 1)

        for j in range(1, ITERS):
            sweep(r, k + j)
            if j == 1:
                @pl.when(r < R - 1)
                def _():
                    coef(r + 1)
        put_out(r, 0)
        seen = jnp.dot(pick_rows, PB[k + ITERS].reshape(X * Z, Y), precision=EXACT)
        predicted = jnp.sum(seen * pick_cols, axis=1, keepdims=True)
        gap = predicted - column(SM[r], 1 + t)
        ES[...] = ES[...] + owned * gap * gap
        return carry

    lax.fori_loop(0, R, step, 0)

    E0[...] = jnp.broadcast_to(jnp.sum(ES[...], axis=0, keepdims=True), E0.shape)
    others = [(d, lax.rem(i + d, N)) for d in range(1, N)]
    for d, peer in others:
        rdma(E0, E1.at[i], s1.at[d], r1.at[i], (t, peer)).start()
    transport(R - 1, True)
    E1[i] = E0[...]
    for d, peer in others:
        rdma(E1.at[peer], E1.at[peer], s1.at[d], r1.at[peer], (t, peer)).wait_recv()
    whole = E1[0]
    for n in range(1, N):
        whole = whole + E1[n]
    mine = lax.broadcasted_iota(jnp.int32, whole.shape, 1) == t
    E2[t] = jnp.where(mine, whole, 0.0)
    for d, peer in peers():
        rdma(E2.at[t], E2.at[t], s2.at[d], r2.at[t], (peer, i)).start()
    for d, peer in peers():
        rdma(E2.at[peer], E2.at[peer], s2.at[d], r2.at[peer], (peer, i)).wait_recv()
    result = E2[0]
    for n in range(1, T):
        result = result + E2[n]
    mis[...] = result * (1.0 / (R * W))

    for side in (0, 1):
        edge_sent(side, M.at[t, edge[side]], MH.at[t], sMH.at[0], rMH.at[t])
        edge_sent(side, PM.at[edge[side]], PH, sPH, rPH)

        def sent_k(k, c):
            edge_sent(side, PB.at[k, edge[side]], HP.at[k], sHP.at[k], rHP.at[k])
            return c

        lax.fori_loop(0, K + 1, sent_k, 0)

        def sent_r(r, c):
            edge_sent(side, FE.at[r, edge[side]], HF.at[r], sHF.at[r], rHF.at[r])

            @pl.when(jnp.logical_and(passes_on(r), has[side]))
            def _():
                rdma(
                    MH.at[r, side], MH.at[r, side], fMH.at[r, side], rMH.at[r, side], (mate, i)
                ).wait_send()
            return c

        lax.fori_loop(0, R, sent_r, 0)
        for d, peer in targets():
            edge_sent(side, M.at[t, edge[side]], MH.at[t], sMH.at[d + 1], rMH.at[t], peer)

    def sent_on(r, c):
        @pl.when(passes_on(r))
        def _():
            rdma(M.at[r], M.at[r], fM.at[r], rM.at[r], (mate, i)).wait_send()
            rdma(I.at[r], I.at[r], fI.at[r], rI.at[r], (mate, i)).wait_send()
        return c

    lax.fori_loop(0, R, sent_on, 0)
    for d, peer in targets():
        rdma(M.at[t], M.at[t], sM.at[d], rM.at[t], (peer, i)).wait_send()
        rdma(I.at[t], I.at[t], sI.at[d], rI.at[t], (peer, i)).wait_send()
    for d, peer in peers():
        rdma(small, SM.at[t], sS.at[d], rS.at[t], (peer, i)).wait_send()
        rdma(E2.at[t], E2.at[t], s2.at[d], r2.at[t], (peer, i)).wait_send()
    for d, peer in others:
        rdma(E0, E1.at[i], s1.at[d], r1.at[i], (t, peer)).wait_send()
    for which in range(len(parts)):
        for d, peer in peers():
            src, dst = piece(which, peer, t)
            rdma(src, dst, sO.at[peer, which], rO.at[t, which], (peer, i)).wait_send()
            src, dst = piece(which, t, peer)
            rdma(src, dst, sO.at[peer, which], rO.at[peer, which], (peer, i)).wait_recv()
        src, dst = piece(which, t, t)
        pltpu.make_async_copy(src, dst, lO.at[which]).wait()


def body(
    perm_field, step_multiplier, inflow, start_pressure, start_saturation,
    region_ids, region_table, well_cells, well_rates, observed,
):
    T = lax.axis_size("tm")
    N = lax.axis_size("space")
    X, Z, Y = start_pressure.shape
    W = well_cells.shape[0]
    members = perm_field.shape[0]
    assert members == T and T % 2 == 0 and step_multiplier.shape[0] == 1
    well_row = (well_cells // Y).astype(jnp.float32)
    well_col = (well_cells % Y).astype(jnp.float32)
    small = jnp.concatenate(
        [well_rates, observed[:, 0, :], well_row[None], well_col[None]], axis=0
    ).T
    small = jnp.pad(small, ((0, 0), (0, 128 - small.shape[1])))
    K = T * ITERS
    f32 = jnp.float32
    cell = (Z, Y)
    block = (X, Z, Y)

    def buf(*shape):
        return pltpu.VMEM(shape, f32)

    dma = pltpu.SemaphoreType.DMA
    vmem = pl.BlockSpec(memory_space=pltpu.VMEM)
    anyspace = pl.BlockSpec(memory_space=pl.ANY)
    out_shape = jax.ShapeDtypeStruct((1, members) + block, f32)
    mis, outp, outs = pl.pallas_call(
        functools.partial(kernel, T, N),
        out_shape=(jax.ShapeDtypeStruct((8, 128), f32), out_shape, out_shape),
        in_specs=[anyspace] * 6 + [pl.BlockSpec(memory_space=pltpu.SMEM)] + [vmem] * 2,
        out_specs=(vmem, anyspace, anyspace),
        scratch_shapes=[
            buf(*block), pltpu.VMEM(block, jnp.int32),
            buf(T, *block), buf(T, *block), buf(T, W, 128), buf(T, 2, *cell), buf(2, *cell),
            buf(K + 1, 2, *cell), buf(T, 2, *cell), buf(K + 1, *block), buf(T + 1, *block),
            buf(T + 1, *block), buf(2, X + 1, *cell), buf(2, *block), buf(2, *block),
            buf(2, *block), buf(2, *block), buf(2, *block), buf(*block), buf(*block), buf(*block),
            buf(*block), buf(2, *block), buf(8, 128), buf(N, 8, 128), buf(T, 8, 128), buf(W, 1),
            dma((T,)), dma((T,)), dma((T,)), dma((T,)), dma((T,)), dma((T,)),
            dma((T, 2)), dma((T, 2)), dma((2,)), dma((2,)), dma((K + 1, 2)), dma((K + 1, 2)),
            dma((T, 2)), dma((T, 2)), dma((T, 4)), dma((T, 4)), dma((4,)),
            dma((N,)), dma((N,)), dma((T,)), dma((T,)),
            dma((T,)), dma((T,)), dma((T, 2)), dma((6,)),
        ],
        compiler_params=pltpu.CompilerParams(
            has_side_effects=True, collective_id=0
        ),
    )(
        perm_field, step_multiplier, inflow, start_pressure, start_saturation, region_ids,
        region_table, small, well_row[None],
    )
    return mis[0, :members], outp, outs


def solution(mesh):
    return jax.shard_map(
        body,
        mesh=mesh,
        in_specs=(
            P(None, "space", None, None),
            P("tm", "space", None, None),
            P("tm", "space", None, None),
            P("space", None, None),
            P("space", None, None),
            P("space", None, None),
            P(),
            P(),
            P("tm", None),
            P(None, "tm", None),
        ),
        out_specs=(P(), P("tm", None, "space", None, None), P("tm", None, "space", None, None)),
        check_vma=False,
    )
```

```python
import functools

import jax
import jax.numpy as jnp
from jax import lax
from jax.experimental import pallas as pl
from jax.experimental.pallas import tpu as pltpu
from jax.sharding import PartitionSpec as P

ITERS = 3
MESH = pl.DeviceIdType.MESH
EXACT = lax.Precision.HIGHEST


def before(v, axis):
    return pltpu.roll(v, 1, axis)


def after(v, axis):
    return pltpu.roll(v, v.shape[axis] - 1, axis)


def kernel(
    T, N,
    perm, mult, infl, p0, s0, ids, table, small, rows_row,
    mis, outp, outs,
    PM, IDS, IH, M, I, SM, MH, PH, HP, HF, PB, SB, FE, TX, TZP, TZM, TYP, TYM, RC, C, V, G, B, Q, E0, E1, E2, ES,
    sM, rM, sI, rI, sS, rS, sMH, rMH, sPH, rPH, sHP, rHP, sHF, rHF, sO, rO, lO, s1, r1, s2, r2,
    fM, fI, fMH, lIN, sIH, rIH, fIH, sC, rC,
):
    t = lax.axis_index("tm")
    i = lax.axis_index("space")
    X, Z, Y = IDS.shape
    R = T
    loads = [
        pltpu.make_async_copy(src, dst, lIN.at[n])
        for n, (src, dst) in enumerate((
            (mult.at[0], M.at[t]), (p0, PB.at[0]), (perm.at[t], PM), (infl.at[0], I.at[t]),
            (ids, IDS), (s0, SB.at[0]),
        ))
    ]
    for load in loads:
        load.start()
    W = small.shape[0]
    K = R * ITERS
    has = (i > 0, i < N - 1)
    beside = (i - 1, i + 1)
    edge = (0, X - 1)
    two = (pl.ds(0, 2), pl.ds(X - 2, 2))
    order = [0, X - 1] + list(range(1, X - 1))

    def rdma(src, dst, ss, rs, dev):
        return pltpu.make_async_remote_copy(
            src_ref=src, dst_ref=dst, send_sem=ss, recv_sem=rs, device_id=dev, device_id_type=MESH
        )

    def halo(side, src, dst_slots, ss, rs, peer=None):
        return rdma(
            src, dst_slots.at[1 - side], ss.at[side], rs.at[1 - side],
            (t if peer is None else peer, beside[side]),
        )

    def send_edge(side, src, slots, ss, rs, peer=None):
        @pl.when(has[side])
        def _():
            halo(side, src, slots, ss, rs, peer).start()

    def edge_sent(side, src, slots, ss, rs, peer=None):
        @pl.when(has[side])
        def _():
            halo(side, src, slots, ss, rs, peer).wait_send()

    def edge_here(side, slots, ss, rs):
        @pl.when(has[side])
        def _():
            rdma(slots.at[side], slots.at[side], ss.at[side], rs.at[side], (t, beside[side])).wait_recv()

    def peers():
        return [(d, lax.rem(t + d, T)) for d in range(1, T)]

    barrier = pltpu.get_barrier_semaphore()

    def greet(device):
        pl.semaphore_signal(barrier, inc=1, device_id=device, device_id_type=MESH)

    for d, peer in peers():
        greet((peer, i))
    for d in range(1, N):
        greet((t, lax.rem(i + d, N)))
    for side in (0, 1):
        @pl.when(has[side])
        def _():
            for d, peer in peers():
                greet((peer, beside[side]))

    sides = jnp.where(has[0], 1, 0) + jnp.where(has[1], 1, 0)
    pl.semaphore_wait(barrier, (N - 1) + (T - 1) + (T - 1) * sides)

    mate = t + 1 - 2 * lax.rem(t, 2)

    def targets():
        return [(0, mate)] + [(d, lax.rem(t + 2 * d, T)) for d in range(1, T // 2)]

    def send_fields():
        for d, peer in targets():
            rdma(M.at[t], M.at[t], sM.at[d], rM.at[t], (peer, i)).start()
        for side in (0, 1):
            for d, peer in targets():
                send_edge(side, M.at[t, two[side]], MH.at[t], sMH.at[d + 1], rMH.at[t], peer)
                send_edge(side, I.at[t, edge[side]], IH.at[t], sIH.at[d + 1], rIH.at[t], peer)
        for d, peer in targets():
            rdma(I.at[t], I.at[t], sI.at[d], rI.at[t], (peer, i)).start()

    def passes_on(r):
        return jnp.logical_and(lax.rem(t, 2) == lax.rem(r, 2), t != r)

    def pass_on(r):
        @pl.when(passes_on(r))
        def _():
            rdma(M.at[r], M.at[r], sM.at[1], rM.at[r], (r, i)).wait_recv()
            rdma(M.at[r], M.at[r], fM.at[r], rM.at[r], (mate, i)).start()
            for side in (0, 1):
                edge_here(side, MH.at[r], sMH.at[0], rMH.at[r])

                @pl.when(has[side])
                def _():
                    rdma(
                        MH.at[r, side], MH.at[r, side], fMH.at[r, side], rMH.at[r, side], (mate, i)
                    ).start()
                edge_here(side, IH.at[r], sIH.at[0], rIH.at[r])

                @pl.when(has[side])
                def _():
                    rdma(
                        IH.at[r, side], IH.at[r, side], fIH.at[r, side], rIH.at[r, side], (mate, i)
                    ).start()
            rdma(I.at[r], I.at[r], sI.at[1], rI.at[r], (r, i)).wait_recv()
            rdma(I.at[r], I.at[r], fI.at[r], rI.at[r], (mate, i)).start()

    for n in range(3):
        loads[n].wait()
    loads[3].wait()
    for side in (0, 1):
        send_edge(side, M.at[t, two[side]], MH.at[t], sMH.at[0], rMH.at[t])
        send_edge(side, I.at[t, edge[side]], IH.at[t], sIH.at[0], rIH.at[t])

    @pl.when(t == 0)
    def _():
        send_fields()

    for side in (0, 1):
        send_edge(side, PM.at[two[side]], PH, sPH, rPH)
        send_edge(side, PB.at[0, two[side]], HP.at[0], sHP.at[0], rHP.at[0])
    for d, peer in peers():
        rdma(small, SM.at[t], sS.at[d], rS.at[t], (peer, i)).start()

    for side in (0, 1):
        @pl.when(jnp.logical_not(has[side]))
        def _():
            zero = jnp.zeros((Z, Y), jnp.float32)
            PH[side] = jnp.zeros((2, Z, Y), jnp.float32)
            C[(0, X + 1)[side]] = zero + 1.0

            def clear(n, c):
                HP[n, side] = jnp.zeros((2, Z, Y), jnp.float32)
                return c

            lax.fori_loop(0, K + 1, clear, 0)

            def clear_r(n, c):
                HF[n, side] = zero
                MH[n, side] = jnp.zeros((2, Z, Y), jnp.float32)
                IH[n, side] = zero
                return c

            lax.fori_loop(0, R, clear_r, 0)

    SM[t] = small[...]
    loads[4].wait()
    loads[5].wait()

    def fraction(s, v):
        sq = s * s
        rest = (1.0 - s) * (1.0 - s)
        return sq / (sq + v * rest)

    for x in order:
        rock = IDS[x]
        c = jnp.zeros((Z, Y), jnp.float32)
        v = c
        g = c
        for k in range(table.shape[1]):
            hit = rock == k
            c = jnp.where(hit, table[0, k], c)
            v = jnp.where(hit, table[1, k], v)
            g = jnp.where(hit, table[2, k], g)
        C[x + 1] = c
        V[x] = v
        G[x] = 0.1 * g
        FE[0, x] = fraction(SB[0, x], v)
    for side in (0, 1):
        send_edge(side, FE.at[0, edge[side]], HF.at[0], sHF.at[0], rHF.at[0])

    def storage_edge(side):
        return rdma(
            C.at[edge[side] + 1], C.at[(X + 1, 0)[side]], sC.at[side], rC.at[1 - side],
            (t, beside[side]),
        )

    for side in (0, 1):
        @pl.when(has[side])
        def _():
            storage_edge(side).start()

    lane = lax.broadcasted_iota(jnp.int32, (W, small.shape[1]), 1)

    def column(block, n):
        return jnp.sum(jnp.where(lane == n, block, 0.0), axis=1, keepdims=True)

    base = (i * (X * Z)).astype(jnp.float32)
    local_col = column(small[...], T + 1) - base
    cols = column(small[...], T + 2)
    pick_rows = jnp.where(
        lax.broadcasted_iota(jnp.int32, (W, X * Z), 1).astype(jnp.float32) == local_col, 1.0, 0.0
    )
    pick_cols = jnp.where(
        lax.broadcasted_iota(jnp.int32, (W, Y), 1).astype(jnp.float32) == cols, 1.0, 0.0
    )
    put_rows = jnp.where(
        lax.broadcasted_iota(jnp.int32, ((X + 2) * Z, W), 0).astype(jnp.float32)
        == rows_row[...] - base + float(Z),
        1.0, 0.0,
    )
    owned = jnp.sum(pick_rows, axis=1, keepdims=True)

    def tm_here(r, buf, ss, rs):
        @pl.when(r != t)
        def _():
            rdma(buf.at[r], buf.at[r], ss.at[1], rs.at[r], (r, i)).wait_recv()

    zi = lax.broadcasted_iota(jnp.int32, (Z, Y), 0)
    yi = lax.broadcasted_iota(jnp.int32, (Z, Y), 1)

    def coef(r):
        slot = lax.rem(r, 2)
        tm_here(r, SM, sS, rS)

        @pl.when(jnp.logical_not(passes_on(r)))
        def _():
            tm_here(r, M, sM, rM)
            for side in (0, 1):
                edge_here(side, MH.at[r], sMH.at[0], rMH.at[r])
                edge_here(side, IH.at[r], sIH.at[0], rIH.at[r])

        a = [PH[0, n] * MH[r, 0, n] for n in (0, 1)]
        a = a + [PM[x] * M[r, x] for x in range(X)] + [PH[1, n] * MH[r, 1, n] for n in (0, 1)]
        for x in range(X + 3):
            TX[slot, x] = jnp.sqrt(a[x] * a[x + 1])
        for x in range(X + 2):
            mid = a[x + 1]
            zp = jnp.where(zi < Z - 1, jnp.sqrt(mid * after(mid, 0)), 0.0)
            yp = jnp.where(yi < Y - 1, jnp.sqrt(mid * after(mid, 1)), 0.0)
            zm = before(zp, 0)
            ym = before(yp, 1)
            TZP[slot, x] = zp
            TZM[slot, x] = zm
            TYP[slot, x] = yp
            TYM[slot, x] = ym
            RC[slot, x] = 1.0 / (C[x] + (TX[slot, x] + TX[slot, x + 1] + zp + zm + yp + ym))
        rate = column(SM[r], 0)
        Q[slot] = jnp.dot(put_rows, pick_cols * rate, precision=EXACT).reshape(X + 2, Z, Y)

    def start_step(r):
        slot = lax.rem(r, 2)

        @pl.when(jnp.logical_not(passes_on(r)))
        def _():
            tm_here(r, I, sI, rI)

        for x in range(X):
            B[x + 1] = C[x + 1] * PB[r * ITERS, x] + Q[slot, x + 1] + I[r, x]

    def layer(k, x):
        if x < 0:
            return HP[k, 0, x + 2]
        return HP[k, 1, x - X] if x >= X else PB[k, x]

    def relaxed(slot, k, x):
        n = x + 1
        p = layer(k, x)
        total = B[n] + TX[slot, n] * layer(k, x - 1) + TX[slot, n + 1] * layer(k, x + 1)
        total = total + TZP[slot, n] * after(p, 0) + TZM[slot, n] * before(p, 0)
        total = total + TYP[slot, n] * after(p, 1) + TYM[slot, n] * before(p, 1)
        return total * RC[slot, n]

    def sweep_wide(r, k):
        slot = lax.rem(r, 2)
        for x in range(1, X - 1):
            PB[k + 1, x] = relaxed(slot, k, x)
        for side in (0, 1):
            edge_here(side, HP.at[k], sHP.at[k], rHP.at[k])
            x = edge[side]
            PB[k + 1, x] = relaxed(slot, k, x)
            x = (-1, X)[side]
            near = HP[k, side, 1 - side]
            B[x + 1] = C[x + 1] * near + Q[slot, x + 1] + IH[r, side]
            HP[k + 1, side, 1 - side] = relaxed(slot, k, x)

    def near_edge(side, k):
        return rdma(
            PB.at[k, edge[side]], HP.at[k, 1 - side, side], sHP.at[k, side], rHP.at[k, 1 - side],
            (t, beside[side]),
        )

    def sweep_plain(r, k):
        slot = lax.rem(r, 2)
        for n, x in enumerate(order):
            PB[k + 1, x] = relaxed(slot, k, x)
            if n < 2:
                @pl.when(has[n])
                def _():
                    near_edge(n, k + 1).start()

    def sweep_last(r, k):
        slot = lax.rem(r, 2)
        for x in range(1, X - 1):
            PB[k + 1, x] = relaxed(slot, k, x)
        for side in (0, 1):
            @pl.when(has[side])
            def _():
                near = HP.at[k, side, 1 - side]
                rdma(near, near, sHP.at[k, side], rHP.at[k, side], (t, beside[side])).wait_recv()

            x = edge[side]
            PB[k + 1, x] = relaxed(slot, k, x)
            send_edge(side, PB.at[k + 1, two[side]], HP.at[k + 1], sHP.at[k + 1], rHP.at[k + 1])

    parts = ((0, 0, X), (1, 1, X - 2), (2, 0, 1), (3, X - 1, 1))

    def piece(which, r, member):
        _, at, many = parts[which]
        rows = pl.ds(at, many)
        if which == 0:
            return PB.at[(r + 1) * ITERS, rows], outp.at[0, member, rows]
        return SB.at[r + 1, rows], outs.at[0, member, rows]

    def put_out(r, which):
        src, dst = piece(which, r, t)

        @pl.when(r != t)
        def _():
            rdma(src, dst, sO.at[r, which], rO.at[t, which], (r, i)).start()

        @pl.when(r == t)
        def _():
            pltpu.make_async_copy(src, dst, lO.at[which]).start()

    def transport(r, last=False):
        slot = lax.rem(r, 2)
        k = (r + 1) * ITERS
        def face(coupling, pi, pj, fi, fj):
            flux = coupling * (pi - pj)
            return flux * jnp.where(flux > 0, fi, fj)

        def p_of(x):
            return layer(k, x)

        def f_of(x):
            return HF[r, 0] if x < 0 else (HF[r, 1] if x >= X else FE[r, x])

        for x in order[2:] + order[:2]:
            if x in edge:
                side = edge.index(x)
                if side == 0:
                    put_out(r, 1)
                edge_here(side, HF.at[r], sHF.at[r], rHF.at[r])
                if last:
                    edge_here(side, HP.at[k], sHP.at[k], rHP.at[k])
            p = p_of(x)
            f = f_of(x)
            s = SB[r, x]
            q = Q[slot, x + 1]
            out = face(TX[slot, x + 2], p, p_of(x + 1), f, f_of(x + 1))
            out = out - face(TX[slot, x + 1], p_of(x - 1), p, f_of(x - 1), f)
            cz = face(TZP[slot, x + 1], p, after(p, 0), f, after(f, 0))
            cy = face(TYP[slot, x + 1], p, after(p, 1), f, after(f, 1))
            out = out + (cz - before(cz, 0)) + (cy - before(cy, 1))
            gained = jnp.maximum(q, 0.0) * (1.0 - s) - jnp.maximum(-q, 0.0) * f - out
            s = s + G[x] * gained
            SB[r + 1, x] = s
            if not last:
                FE[r + 1, x] = fraction(s, V[x])
            if x in edge:
                put_out(r, 2 + edge.index(x))

        @pl.when(r < R - 1)
        def _():
            for side in (0, 1):
                send_edge(side, FE.at[r + 1, edge[side]], HF.at[r + 1], sHF.at[r + 1], rHF.at[r + 1])

    pass_on(0)

    @pl.when(t > 0)
    def _():
        send_fields()

    for side in (0, 1):
        edge_here(side, PH, sPH, rPH)

        @pl.when(has[side])
        def _():
            storage = C.at[(0, X + 1)[side]]
            rdma(storage, storage, sC.at[side], rC.at[side], (t, beside[side])).wait_recv()
    coef(0)
    ES[...] = jnp.zeros(ES.shape, jnp.float32)

    def step(r, carry):
        k = r * ITERS
        start_step(r)
        sweep_wide(r, k)
        sweep_plain(r, k + 1)

        @pl.when(r > 0)
        def _():
            transport(r - 1)

        @pl.when(r < R - 1)
        def _():
            pass_on(r + 1)

        sweep_last(r, k + 2)

        @pl.when(r < R - 1)
        def _():
            coef(r + 1)

        put_out(r, 0)
        seen = jnp.dot(pick_rows, PB[k + ITERS].reshape(X * Z, Y), precision=EXACT)
        predicted = jnp.sum(seen * pick_cols, axis=1, keepdims=True)
        gap = predicted - column(SM[r], 1 + t)
        ES[...] = ES[...] + owned * gap * gap
        return carry

    lax.fori_loop(0, R, step, 0)

    E0[...] = jnp.broadcast_to(jnp.sum(ES[...], axis=0, keepdims=True), E0.shape)
    others = [(d, lax.rem(i + d, N)) for d in range(1, N)]
    for d, peer in others:
        rdma(E0, E1.at[i], s1.at[d], r1.at[i], (t, peer)).start()
    transport(R - 1, True)
    E1[i] = E0[...]
    for d, peer in others:
        rdma(E1.at[peer], E1.at[peer], s1.at[d], r1.at[peer], (t, peer)).wait_recv()
    whole = E1[0]
    for n in range(1, N):
        whole = whole + E1[n]
    mine = lax.broadcasted_iota(jnp.int32, whole.shape, 1) == t
    E2[t] = jnp.where(mine, whole, 0.0)
    for d, peer in peers():
        rdma(E2.at[t], E2.at[t], s2.at[d], r2.at[t], (peer, i)).start()
    for d, peer in peers():
        rdma(E2.at[peer], E2.at[peer], s2.at[d], r2.at[peer], (peer, i)).wait_recv()
    result = E2[0]
    for n in range(1, T):
        result = result + E2[n]
    mis[...] = result * (1.0 / (R * W))

    for side in (0, 1):
        edge_sent(side, M.at[t, two[side]], MH.at[t], sMH.at[0], rMH.at[t])
        edge_sent(side, I.at[t, edge[side]], IH.at[t], sIH.at[0], rIH.at[t])
        edge_sent(side, PM.at[two[side]], PH, sPH, rPH)

        @pl.when(has[side])
        def _():
            storage_edge(side).wait_send()

        def sent_k(k, c):
            k = k * ITERS
            edge_sent(side, PB.at[k, two[side]], HP.at[k], sHP.at[k], rHP.at[k])
            return c

        lax.fori_loop(0, R + 1, sent_k, 0)

        def sent_n(r, c):
            @pl.when(has[side])
            def _():
                near_edge(side, r * ITERS + 2).wait_send()
            return c

        lax.fori_loop(0, R, sent_n, 0)

        def sent_r(r, c):
            edge_sent(side, FE.at[r, edge[side]], HF.at[r], sHF.at[r], rHF.at[r])

            @pl.when(jnp.logical_and(passes_on(r), has[side]))
            def _():
                rdma(
                    MH.at[r, side], MH.at[r, side], fMH.at[r, side], rMH.at[r, side], (mate, i)
                ).wait_send()
                rdma(
                    IH.at[r, side], IH.at[r, side], fIH.at[r, side], rIH.at[r, side], (mate, i)
                ).wait_send()
            return c

        lax.fori_loop(0, R, sent_r, 0)
        for d, peer in targets():
            edge_sent(side, M.at[t, two[side]], MH.at[t], sMH.at[d + 1], rMH.at[t], peer)
            edge_sent(side, I.at[t, edge[side]], IH.at[t], sIH.at[d + 1], rIH.at[t], peer)

    def sent_on(r, c):
        @pl.when(passes_on(r))
        def _():
            rdma(M.at[r], M.at[r], fM.at[r], rM.at[r], (mate, i)).wait_send()
            rdma(I.at[r], I.at[r], fI.at[r], rI.at[r], (mate, i)).wait_send()
        return c

    lax.fori_loop(0, R, sent_on, 0)
    for d, peer in targets():
        rdma(M.at[t], M.at[t], sM.at[d], rM.at[t], (peer, i)).wait_send()
        rdma(I.at[t], I.at[t], sI.at[d], rI.at[t], (peer, i)).wait_send()
    for d, peer in peers():
        rdma(small, SM.at[t], sS.at[d], rS.at[t], (peer, i)).wait_send()
        rdma(E2.at[t], E2.at[t], s2.at[d], r2.at[t], (peer, i)).wait_send()
    for d, peer in others:
        rdma(E0, E1.at[i], s1.at[d], r1.at[i], (t, peer)).wait_send()
    for which in range(len(parts)):
        for d, peer in peers():
            src, dst = piece(which, peer, t)
            rdma(src, dst, sO.at[peer, which], rO.at[t, which], (peer, i)).wait_send()
            src, dst = piece(which, t, peer)
            rdma(src, dst, sO.at[peer, which], rO.at[peer, which], (peer, i)).wait_recv()
        src, dst = piece(which, t, t)
        pltpu.make_async_copy(src, dst, lO.at[which]).wait()


def body(
    perm_field, step_multiplier, inflow, start_pressure, start_saturation,
    region_ids, region_table, well_cells, well_rates, observed,
):
    T = lax.axis_size("tm")
    N = lax.axis_size("space")
    X, Z, Y = start_pressure.shape
    W = well_cells.shape[0]
    members = perm_field.shape[0]
    assert members == T and T % 2 == 0 and step_multiplier.shape[0] == 1
    well_row = (well_cells // Y).astype(jnp.float32)
    well_col = (well_cells % Y).astype(jnp.float32)
    small = jnp.concatenate(
        [well_rates, observed[:, 0, :], well_row[None], well_col[None]], axis=0
    ).T
    small = jnp.pad(small, ((0, 0), (0, 128 - small.shape[1])))
    K = T * ITERS
    f32 = jnp.float32
    cell = (Z, Y)
    block = (X, Z, Y)
    wide = (X + 2, Z, Y)

    def buf(*shape):
        return pltpu.VMEM(shape, f32)

    dma = pltpu.SemaphoreType.DMA
    vmem = pl.BlockSpec(memory_space=pltpu.VMEM)
    anyspace = pl.BlockSpec(memory_space=pl.ANY)
    out_shape = jax.ShapeDtypeStruct((1, members) + block, f32)
    mis, outp, outs = pl.pallas_call(
        functools.partial(kernel, T, N),
        out_shape=(jax.ShapeDtypeStruct((8, 128), f32), out_shape, out_shape),
        in_specs=[anyspace] * 6 + [pl.BlockSpec(memory_space=pltpu.SMEM)] + [vmem] * 2,
        out_specs=(vmem, anyspace, anyspace),
        scratch_shapes=[
            buf(*block), pltpu.VMEM(block, jnp.int32), buf(T, 2, *cell),
            buf(T, *block), buf(T, *block), buf(T, W, 128), buf(T, 2, 2, *cell), buf(2, 2, *cell),
            buf(K + 1, 2, 2, *cell), buf(T, 2, *cell), buf(K + 1, *block), buf(T + 1, *block),
            buf(T + 1, *block), buf(2, X + 3, *cell), buf(2, *wide), buf(2, *wide),
            buf(2, *wide), buf(2, *wide), buf(2, *wide), buf(*wide), buf(*block), buf(*block),
            buf(*wide), buf(2, *wide), buf(8, 128), buf(N, 8, 128), buf(T, 8, 128), buf(W, 1),
            dma((T,)), dma((T,)), dma((T,)), dma((T,)), dma((T,)), dma((T,)),
            dma((T, 2)), dma((T, 2)), dma((2,)), dma((2,)), dma((K + 1, 2)), dma((K + 1, 2)),
            dma((T, 2)), dma((T, 2)), dma((T, 4)), dma((T, 4)), dma((4,)),
            dma((N,)), dma((N,)), dma((T,)), dma((T,)),
            dma((T,)), dma((T,)), dma((T, 2)), dma((6,)), dma((T, 2)), dma((T, 2)), dma((T, 2)),
            dma((2,)), dma((2,)),
        ],
        compiler_params=pltpu.CompilerParams(
            has_side_effects=True, collective_id=0
        ),
    )(
        perm_field, step_multiplier, inflow, start_pressure, start_saturation, region_ids,
        region_table, small, well_row[None],
    )
    return mis[0, :members], outp, outs


def solution(mesh):
    return jax.shard_map(
        body,
        mesh=mesh,
        in_specs=(
            P(None, "space", None, None),
            P("tm", "space", None, None),
            P("tm", "space", None, None),
            P("space", None, None),
            P("space", None, None),
            P("space", None, None),
            P(),
            P(),
            P("tm", None),
            P(None, "tm", None),
        ),
        out_specs=(P(), P("tm", None, "space", None, None), P("tm", None, "space", None, None)),
        check_vma=False,
    )
```
